32 devices in a mesh: gx: 32 (over z, y, x, core).
Axes of the slice: x: 2, y: 2, z: 4, core: 2. Of those that a mesh axis runs over, the one named last changes fastest.
Arguments:
- value: float32 [64, 48, 32, 128], P('gx'), may hold values from -6 to 6
- target: float32 [64, 48, 32, 128], P('gx'), may hold values from -6 to 6
- obstacle: float32 [64, 48, 32, 128], P('gx'), may hold values from -6 to -0.5
- fractions: float32 [16, 4], replicated, may hold values from 0 to 1
- control_cost: float32 [16], replicated, may hold values from 0 to 0.5
- shard_offset: int32 [16], replicated, may hold values from -8 to 8, as said below
- cell_offset: int32 [16], replicated, may hold values from 0 to 1
- grid_offset: int32 [16, 3], replicated, may hold values from -4 to 4
Outputs:
- updated: float32 [64, 48, 32, 128], P('gx')
The draws below stay inside these ranges and needn't reach their ends.
Inputs may be any that keep to these rules, and one draw needn't show every extreme that they name: `shard_offset`: every draw holds both -8 and 8.
All inputs are finite; a program needn't handle non-finite values.
Results may differ from the reference program's by a relative error of at most 0.00002.
Values sent between devices are 32-bit elements; how exact they have to be, the bound alone decides.
A program may use at most 128 MiB of HBM per device.

```python
import jax
import jax.numpy as jnp
from jax import lax

CX = 2
NY = 48
NZ = 32
NW = 128
NCTRL = 16
REACH = 8
NX = 64


def draw_shard_offset(key, part):
    first_key, second_key = jax.random.split(jax.random.fold_in(key, 11))
    offsets = jax.random.randint(first_key, (NCTRL,), -REACH, REACH + 1)
    order = jax.random.permutation(second_key, NCTRL)
    offsets = offsets.at[order[0]].set(-REACH).at[order[1]].set(REACH)
    return offsets.astype(jnp.int32)


def set_ends(entries, own_key, smallest, top_value):
    index_at = [jax.random.randint(jax.random.fold_in(own_key, axis), (), 0, length) for axis, length in enumerate(entries.shape)]
    widest = entries.shape.index(max(entries.shape))
    neighbour = index_at[:widest] + [(index_at[widest] + 1) % entries.shape[widest]] + index_at[widest + 1:]
    return entries.at[tuple(index_at)].set(smallest).at[tuple(neighbour)].set(top_value)


def block_levels(own_key, shape, cuts, low, high):
    def one(axis_at, blocks):
        heights = jax.random.uniform(jax.random.fold_in(jax.random.fold_in(own_key, 6), axis_at), (blocks,), jnp.float32, low / len(cuts), high / len(cuts))
        return jnp.repeat(jnp.exp(heights), shape[axis_at] // blocks).reshape((-1,) + (1,) * (len(shape) - axis_at - 1))

    level = one(*cuts[0])
    for cut in cuts[1:]:
        level = level * one(*cut)
    return level


def bell_draw(own_key, extent, width, reach, cuts=(), held_as=jnp.bfloat16):
    gain = block_levels(own_key, extent, cuts, -0.22, 0.18) if cuts else 1.0
    array = jax.random.normal(own_key, extent, jnp.float32) * width * gain
    return jnp.minimum(jnp.maximum(array, -reach), reach).astype(held_as)


def setup_inputs(seed: int = 0) -> dict:
    arg_keys = jax.random.split(jax.random.key(seed), 9)
    value = bell_draw(arg_keys[0], (NX, NY, NZ, NW), 1.0, 6.0, ((0, 32),), jnp.float32)
    target = bell_draw(arg_keys[1], (NX, NY, NZ, NW), 1.0, 6.0, ((0, 32),), jnp.float32)
    obstacle = jnp.clip(-6.0 + 5.5 * jax.random.uniform(arg_keys[2], (NX, NY, NZ, NW), jnp.float32) ** block_levels(arg_keys[2], (NX, NY, NZ, NW), ((0, 32),), -0.2, 0.2), -6.0, -0.5)
    fractions = jnp.clip(jax.random.uniform(arg_keys[3], (NCTRL, 4), jnp.float32, 0.0, 1.0), 0.0, 1.0)
    control_cost = jnp.clip(jax.random.uniform(arg_keys[4], (NCTRL,), jnp.float32, 0.0, 0.5), 0.0, 0.5)
    shard_offset = draw_shard_offset(jax.random.fold_in(arg_keys[8], 71), 0)
    cell_offset = set_ends(jax.random.randint(arg_keys[6], (NCTRL,), 0, CX), jax.random.fold_in(arg_keys[6], 1), 0, CX - 1).astype(jnp.int32)
    grid_offset = set_ends(jax.random.randint(arg_keys[7], (NCTRL, 3), -4, 5), jax.random.fold_in(arg_keys[7], 1), -4, 4).astype(jnp.int32)
    return {"value": value, "target": target, "obstacle": obstacle, "fractions": fractions, "control_cost": control_cost, "shard_offset": shard_offset, "cell_offset": cell_offset, "grid_offset": grid_offset}


def blend(low, high, frac):
    return (1.0 - frac) * low + frac * high


def reference(value, target, obstacle, fractions, control_cost, shard_offset, cell_offset, grid_offset):
    def one_control(u, best):
        along = (shard_offset[u] * CX + cell_offset[u]).astype(jnp.int32)
        field = blend(jnp.roll(value, -along, axis=0), jnp.roll(value, -along - 1, axis=0), fractions[u, 0])
        for axis_k in range(1, 4):
            moved = grid_offset[u, axis_k - 1].astype(jnp.int32)
            field = blend(jnp.roll(field, -moved, axis=axis_k), jnp.roll(field, -moved - 1, axis=axis_k), fractions[u, axis_k])
        return jnp.minimum(best, field + control_cost[u])

    start = jnp.full(value.shape, jnp.inf, jnp.float32)
    best = lax.fori_loop(0, NCTRL, one_control, start)
    return jnp.maximum(obstacle, jnp.minimum(target, best))
```

```python
import functools

import jax
import jax.numpy as jnp
from jax import lax
from jax.experimental import pallas as pl
from jax.experimental.pallas import tpu as pltpu
from jax.sharding import PartitionSpec as P

GROUP = 8
MESH = pl.DeviceIdType.MESH
HALVES = 2
UNROLL = 4


def gather_kernel(n, value_ref, out_ref, send_sem, recv_sem, own_sem):
    me = lax.axis_index("gx")
    j = lax.rem(me, GROUP)
    base = me - j
    core = lax.rem(j, 2)

    def xor(bits):
        got = j
        for bit in (1, 2, 4):
            if bits & bit:
                got = got + bit - 2 * bit * lax.rem(got // bit, 2)
        return got

    mate, xn, yn, diag = xor(1), xor(2), xor(4), xor(6)
    first, first_to = jnp.where(core == 0, xn, yn), jnp.where(core == 0, yn, xn)
    second = first_to
    down, up = lax.rem(me + n - GROUP, n), lax.rem(me + GROUP, n)

    barrier = pltpu.get_barrier_semaphore()
    for other in (base + mate, base + xn, base + yn, down, up):
        pl.semaphore_signal(barrier, inc=1, device_id=(other,), device_id_type=MESH)
    pl.semaphore_wait(barrier, 5)

    rows, ny = value_ref.shape[0], value_ref.shape[1]
    part = ny // HALVES
    pieces = [(r, pl.ds(h * part, part)) for r in range(rows) for h in range(HALVES)]
    count = len(pieces)

    def copy(src, slot, kind, q, target):
        r, ys = pieces[q]
        return pltpu.make_async_remote_copy(
            src_ref=src.at[r, ys],
            dst_ref=out_ref.at[slot, r, ys],
            send_sem=send_sem.at[kind, q],
            recv_sem=recv_sem.at[slot, q],
            device_id=(target,),
            device_id_type=MESH,
        )

    def arrived(slot, q):
        r, ys = pieces[q]
        ref = out_ref.at[slot, r, ys]
        pltpu.make_async_copy(ref, ref, recv_sem.at[slot, q]).wait()

    def to_halo(slot, src, q):
        @pl.when(slot == 0)
        def _():
            copy(src, GROUP, 7, q, down).start()

    own = pltpu.make_async_copy(value_ref, out_ref.at[j], own_sem)
    for q in range(count):
        copy(value_ref, j, 0, q, base + first).start()
        copy(value_ref, j, 1, q, base + second).start()
        copy(value_ref, j, 2, q, base + mate).start()
        to_halo(j, value_ref, q)
    own.start()

    def take(slot, q, kinds):
        arrived(slot, q)
        src = out_ref.at[slot]
        for kind, target in kinds:
            copy(src, slot, kind, q, base + target).start()
        to_halo(slot, src, q)

    for q in range(count + 2):
        if q < count:
            take(first, q, [(3, first_to), (4, mate)])
            take(second, q, [(5, mate)])
            take(mate, q, [])
        if 1 <= q <= count:
            take(diag, q - 1, [(6, mate)])
            take(xor(3), q - 1, [])
            take(xor(5), q - 1, [])
        if q >= 2:
            take(xor(7), q - 2, [])
    for q in range(count):
        arrived(GROUP, q)
    own.wait()
    for kind in range(8):
        for q in range(count):
            copy(value_ref, j, kind, q, base + mate).wait_send()


def gather(n, value):
    rows = value.shape
    count = rows[0] * HALVES
    return pl.pallas_call(
        functools.partial(gather_kernel, n),
        out_shape=jax.ShapeDtypeStruct((GROUP + 1,) + rows, value.dtype),
        in_specs=[pl.BlockSpec(memory_space=pltpu.VMEM)],
        out_specs=pl.BlockSpec(memory_space=pl.ANY),
        scratch_shapes=[
            pltpu.SemaphoreType.DMA((8, count)),
            pltpu.SemaphoreType.DMA((GROUP + 1, count)),
            pltpu.SemaphoreType.DMA,
        ],
        compiler_params=pltpu.CompilerParams(collective_id=0, has_side_effects=True),
    )(value)


def partial_kernel(side, frac, cost, slab_at, cell_at, grid_at, src, best, held, mid, picked, sem):
    rows, ny, nz, nw = best.shape
    j = lax.rem(lax.axis_index("gx"), GROUP)
    controls = cost.shape[0]

    def place(u):
        return j + slab_at[u] + side * GROUP

    def pick(u, m):
        at = place(u)
        inside = jnp.logical_and(at >= 0, at < GROUP)

        @pl.when(inside)
        def _():
            picked[m] = u

        return m + inside.astype(jnp.int32)

    number = lax.fori_loop(0, controls, pick, 0)
    best[...] = jnp.full(best.shape, jnp.inf, jnp.float32)

    def fetch(i):
        u = picked[i]
        start = place(u) * rows + cell_at[u]
        slot = lax.rem(i, 2)
        return pltpu.make_async_copy(src.at[pl.ds(start, rows + 1)], held.at[slot], sem.at[slot])

    @pl.when(number > 0)
    def _():
        fetch(0).start()

    def one(i, carry):
        @pl.when(i + 1 < number)
        def _():
            fetch(i + 1).start()

        fetch(i).wait()
        slot = lax.rem(i, 2)
        u = picked[i]
        fx, fy, fz, fw = frac[u, 0], frac[u, 1], frac[u, 2], frac[u, 3]
        gy, gz, gw = grid_at[u, 0], grid_at[u, 1], grid_at[u, 2]
        add = cost[u]
        turn = lax.rem(nw - gw, nw)
        turn1 = lax.rem(nw - gw - 1, nw)

        def row(r, c):
            def along(y):
                y = y + gy
                y = jnp.where(y < 0, y + ny, y)
                y = jnp.where(y >= ny, y - ny, y)
                low, high = held[slot, r, y], held[slot, r + 1, y]
                return low + fx * (high - low)

            def first(b, low):
                for k in range(UNROLL):
                    y = b * UNROLL + k
                    high = along(y + 1)
                    got = low + fy * (high - low)
                    mid[y, 8:8 + nz] = got
                    mid[y, 0:8] = got[nz - 8:]
                    mid[y, 8 + nz:16 + nz] = got[:8]
                    low = high
                return low

            lax.fori_loop(0, ny // UNROLL, first, along(0))

            def second(b, c2):
                for k in range(UNROLL):
                    y = b * UNROLL + k
                    low = mid[y, pl.ds(8 + gz, nz)]
                    high = mid[y, pl.ds(9 + gz, nz)]
                    got = low + fz * (high - low)
                    low, high = pltpu.roll(got, turn, 1), pltpu.roll(got, turn1, 1)
                    got = low + fw * (high - low) + add
                    best[r, y] = jnp.minimum(best[r, y], got)
                return c2

            lax.fori_loop(0, ny // UNROLL, second, 0)
            return c

        return lax.fori_loop(0, rows, row, carry)

    lax.fori_loop(0, number, one, 0)


def partial(side, like, src, frac, cost, slab_at, cell_at, grid_at):
    rows, ny, nz, nw = like.shape
    smem = pl.BlockSpec(memory_space=pltpu.SMEM)
    flat = src.reshape((src.shape[0] * rows, ny, nz, nw))
    return pl.pallas_call(
        functools.partial(partial_kernel, side),
        out_shape=jax.ShapeDtypeStruct(like.shape, like.dtype),
        in_specs=[smem] * 5 + [pl.BlockSpec(memory_space=pl.ANY)],
        out_specs=pl.BlockSpec(memory_space=pltpu.VMEM),
        scratch_shapes=[
            pltpu.VMEM((2, rows + 1, ny, nz, nw), jnp.float32),
            pltpu.VMEM((ny, nz + 16, nw), jnp.float32),
            pltpu.SMEM((cost.shape[0],), jnp.int32),
            pltpu.SemaphoreType.DMA((2,)),
        ],
        cost_estimate=pl.CostEstimate(flops=30000000, bytes_accessed=20000000, transcendentals=0),
    )(frac, cost, slab_at, cell_at, grid_at, flat)


def passed_along(x, by):
    size = lax.axis_size("gx")
    return lax.ppermute(x, "gx", [(i, (i + by) % size) for i in range(size)])


def body(value, target, obstacle, *params):
    n = lax.axis_size("gx")
    src = gather(n, value)
    below = passed_along(partial(-1, value, src, *params), -GROUP)
    above = passed_along(partial(1, value, src, *params), GROUP)
    own = partial(0, value, src, *params)
    best = jnp.minimum(own, jnp.minimum(below, above))
    return jnp.maximum(obstacle, jnp.minimum(target, best))


def solution(mesh):
    slab = P("gx", None, None, None)
    return jax.shard_map(
        body,
        mesh=mesh,
        in_specs=(slab, slab, slab, P(), P(), P(), P(), P()),
        out_specs=slab,
        check_vma=False,
    )
```

```python
import functools

import jax
import jax.numpy as jnp
from jax import lax
from jax.experimental import pallas as pl
from jax.experimental.pallas import tpu as pltpu
from jax.sharding import PartitionSpec as P

GROUP = 8
MESH = pl.DeviceIdType.MESH
HALVES = 2
UNROLL = 8


def gather_kernel(n, value_ref, out_ref, send_sem, recv_sem, own_sem):
    me = lax.axis_index("gx")
    j = lax.rem(me, GROUP)
    base = me - j
    core = lax.rem(j, 2)

    def xor(bits):
        got = j
        for bit in (1, 2, 4):
            if bits & bit:
                got = got + bit - 2 * bit * lax.rem(got // bit, 2)
        return got

    mate, xn, yn, diag = xor(1), xor(2), xor(4), xor(6)
    first, first_to = jnp.where(core == 0, xn, yn), jnp.where(core == 0, yn, xn)
    second = first_to
    down, up = lax.rem(me + n - GROUP, n), lax.rem(me + GROUP, n)

    barrier = pltpu.get_barrier_semaphore()
    for other in (base + mate, base + xn, base + yn, down, up):
        pl.semaphore_signal(barrier, inc=1, device_id=(other,), device_id_type=MESH)
    pl.semaphore_wait(barrier, 5)

    rows, ny = value_ref.shape[0], value_ref.shape[1]
    part = ny // HALVES
    pieces = [(r, pl.ds(h * part, part)) for r in range(rows) for h in range(HALVES)]
    count = len(pieces)

    def copy(src, slot, kind, q, target):
        r, ys = pieces[q]
        return pltpu.make_async_remote_copy(
            src_ref=src.at[r, ys],
            dst_ref=out_ref.at[slot, r, ys],
            send_sem=send_sem.at[kind, q],
            recv_sem=recv_sem.at[slot, q],
            device_id=(target,),
            device_id_type=MESH,
        )

    def arrived(slot, q):
        r, ys = pieces[q]
        ref = out_ref.at[slot, r, ys]
        pltpu.make_async_copy(ref, ref, recv_sem.at[slot, q]).wait()

    def to_halo(slot, src, q):
        @pl.when(slot == 0)
        def _():
            copy(src, GROUP, 7, q, down).start()

    own = pltpu.make_async_copy(value_ref, out_ref.at[j], own_sem)
    for q in range(count):
        copy(value_ref, j, 0, q, base + first).start()
        copy(value_ref, j, 1, q, base + second).start()
        copy(value_ref, j, 2, q, base + mate).start()
        to_halo(j, value_ref, q)
    own.start()

    def take(slot, q, kinds):
        arrived(slot, q)
        src = out_ref.at[slot]
        for kind, target in kinds:
            copy(src, slot, kind, q, base + target).start()
        to_halo(slot, src, q)

    for q in range(count + 2):
        if q < count:
            take(first, q, [(3, first_to), (4, mate)])
            take(second, q, [(5, mate)])
            take(mate, q, [])
        if 1 <= q <= count:
            take(diag, q - 1, [(6, mate)])
            take(xor(3), q - 1, [])
            take(xor(5), q - 1, [])
        if q >= 2:
            take(xor(7), q - 2, [])
    for q in range(count):
        arrived(GROUP, q)
    own.wait()
    for kind in range(8):
        for q in range(count):
            copy(value_ref, j, kind, q, base + mate).wait_send()


def gather(n, value):
    rows = value.shape
    count = rows[0] * HALVES
    return pl.pallas_call(
        functools.partial(gather_kernel, n),
        out_shape=pltpu.VMEM((GROUP + 1,) + rows, value.dtype),
        in_specs=[pl.BlockSpec(memory_space=pltpu.VMEM)],
        out_specs=pl.BlockSpec(memory_space=pltpu.VMEM),
        scratch_shapes=[
            pltpu.SemaphoreType.DMA((8, count)),
            pltpu.SemaphoreType.DMA((GROUP + 1, count)),
            pltpu.SemaphoreType.DMA,
        ],
        compiler_params=pltpu.CompilerParams(
            collective_id=0, has_side_effects=True, vmem_limit_bytes=20 * 2**20
        ),
    )(value)


def partial_kernel(side, frac, cost, slab_at, cell_at, grid_at, src, best, mid, picked):
    rows, ny, nz, nw = best.shape
    j = lax.rem(lax.axis_index("gx"), GROUP)
    controls = cost.shape[0]

    def place(u):
        return j + slab_at[u] + side * GROUP

    def pick(u, m):
        at = place(u)
        inside = jnp.logical_and(at >= 0, at < GROUP)

        @pl.when(inside)
        def _():
            picked[m] = u

        return m + inside.astype(jnp.int32)

    number = lax.fori_loop(0, controls, pick, 0)
    best[...] = jnp.full(best.shape, jnp.inf, jnp.float32)

    def one(i, carry):
        u = picked[i]
        start = place(u) * rows + cell_at[u]
        fx, fy, fz, fw = frac[u, 0], frac[u, 1], frac[u, 2], frac[u, 3]
        gy, gz, gw = grid_at[u, 0], grid_at[u, 1], grid_at[u, 2]
        add = cost[u]
        turn = lax.rem(nw - gw, nw)
        turn1 = lax.rem(nw - gw - 1, nw)

        def row(r, c):
            def along(y):
                y = y + gy
                y = jnp.where(y < 0, y + ny, y)
                y = jnp.where(y >= ny, y - ny, y)
                low, high = src[start + r, y], src[start + r + 1, y]
                return low + fx * (high - low)

            def first(b, low):
                for k in range(UNROLL):
                    y = b * UNROLL + k
                    high = along(y + 1)
                    got = low + fy * (high - low)
                    mid[y, 8:8 + nz] = got
                    mid[y, 0:8] = got[nz - 8:]
                    mid[y, 8 + nz:16 + nz] = got[:8]
                    low = high
                return low

            lax.fori_loop(0, ny // UNROLL, first, along(0))

            def second(b, c2):
                for k in range(UNROLL):
                    y = b * UNROLL + k
                    low = mid[y, pl.ds(8 + gz, nz)]
                    high = mid[y, pl.ds(9 + gz, nz)]
                    got = low + fz * (high - low)
                    low, high = pltpu.roll(got, turn, 1), pltpu.roll(got, turn1, 1)
                    got = low + fw * (high - low) + add
                    best[r, y] = jnp.minimum(best[r, y], got)
                return c2

            lax.fori_loop(0, ny // UNROLL, second, 0)
            return c

        return lax.fori_loop(0, rows, row, carry)

    lax.fori_loop(0, number, one, 0)


def partial(side, like, src, frac, cost, slab_at, cell_at, grid_at):
    rows, ny, nz, nw = like.shape
    smem = pl.BlockSpec(memory_space=pltpu.SMEM)
    flat = src.reshape((src.shape[0] * rows, ny, nz, nw))
    return pl.pallas_call(
        functools.partial(partial_kernel, side),
        out_shape=jax.ShapeDtypeStruct(like.shape, like.dtype),
        in_specs=[smem] * 5 + [pl.BlockSpec(memory_space=pltpu.VMEM)],
        out_specs=pl.BlockSpec(memory_space=pltpu.VMEM),
        scratch_shapes=[
            pltpu.VMEM((ny, nz + 16, nw), jnp.float32),
            pltpu.SMEM((cost.shape[0],), jnp.int32),
        ],
        compiler_params=pltpu.CompilerParams(vmem_limit_bytes=20 * 2**20),
        cost_estimate=pl.CostEstimate(flops=30000000, bytes_accessed=20000000, transcendentals=0),
    )(frac, cost, slab_at, cell_at, grid_at, flat)


def passed_along(x, by):
    size = lax.axis_size("gx")
    return lax.ppermute(x, "gx", [(i, (i + by) % size) for i in range(size)])


def body(value, target, obstacle, *params):
    n = lax.axis_size("gx")
    src = gather(n, value)
    below = passed_along(partial(-1, value, src, *params), -GROUP)
    above = passed_along(partial(1, value, src, *params), GROUP)
    own = partial(0, value, src, *params)
    best = jnp.minimum(own, jnp.minimum(below, above))
    return jnp.maximum(obstacle, jnp.minimum(target, best))


def solution(mesh):
    slab = P("gx", None, None, None)
    return jax.shard_map(
        body,
        mesh=mesh,
        in_specs=(slab, slab, slab, P(), P(), P(), P(), P()),
        out_specs=slab,
        check_vma=False,
    )
```

```python
import functools

import jax
import jax.numpy as jnp
from jax import lax
from jax.experimental import pallas as pl
from jax.experimental.pallas import tpu as pltpu
from jax.sharding import PartitionSpec as P


GROUP = 8
MESH = pl.DeviceIdType.MESH
SHIFT = 4
PIECE = 17
UNROLL = 8


def pieces_of(rows, low, high):
    parts = -(-(high - low) // PIECE)
    cuts = [low + (high - low) * i // parts for i in range(parts + 1)]
    return [(r, pl.ds(a, b - a)) for r in range(rows) for a, b in zip(cuts, cuts[1:])]


def gather_kernel(n, low, high, value_ref, *refs):
    earlier, (out_ref, send_sem, recv_sem, own_sem) = refs[:-4], refs[-4:]
    me = lax.axis_index("gx")
    j = lax.rem(me, GROUP)
    base = me - j
    core = lax.rem(j, 2)

    def xor(bits):
        got = j
        for bit in (1, 2, 4):
            if bits & bit:
                got = got + bit - 2 * bit * lax.rem(got // bit, 2)
        return got

    mate, xn, yn, diag = xor(1), xor(2), xor(4), xor(6)
    first, first_to = jnp.where(core == 0, xn, yn), jnp.where(core == 0, yn, xn)
    second = first_to
    down, up = lax.rem(me + n - GROUP, n), lax.rem(me + GROUP, n)

    barrier = pltpu.get_barrier_semaphore()
    for other in (base + mate, base + xn, base + yn, down, up):
        pl.semaphore_signal(barrier, inc=1, device_id=(other,), device_id_type=MESH)
    pl.semaphore_wait(barrier, 5)

    rows = value_ref.shape[0]
    pieces = pieces_of(rows, low, high)
    count = len(pieces)

    def copy(src, slot, kind, q, target):
        r, ys = pieces[q]
        return pltpu.make_async_remote_copy(
            src_ref=src.at[r, ys],
            dst_ref=out_ref.at[slot, r, ys],
            send_sem=send_sem.at[kind, q],
            recv_sem=recv_sem.at[slot, q],
            device_id=(target,),
            device_id_type=MESH,
        )

    def arrived(slot, q):
        r, ys = pieces[q]
        ref = out_ref.at[slot, r, ys]
        pltpu.make_async_copy(ref, ref, recv_sem.at[slot, q]).wait()

    def to_halo(slot, src, q):
        @pl.when(jnp.logical_and(slot == 0, core == 0))
        def _():
            copy(src, GROUP, 7, q, down).start()

    local = [
        pltpu.make_async_copy(
            value_ref.at[r, pl.ds(low, high - low)],
            out_ref.at[j, r, pl.ds(low, high - low)],
            own_sem.at[r],
        )
        for r in range(rows)
    ]
    for ref in earlier:
        local += [
            pltpu.make_async_copy(
                ref.at[slot, r], out_ref.at[slot, r, pl.ds(0, low)], own_sem.at[rows * (slot + 1) + r]
            )
            for slot in range(GROUP + 1)
            for r in range(rows)
        ]
    for q in range(count):
        copy(value_ref, j, 0, q, base + first).start()
        copy(value_ref, j, 1, q, base + second).start()
        copy(value_ref, j, 2, q, base + mate).start()
        to_halo(j, value_ref, q)
    for c in local:
        c.start()

    def take(slot, q, kinds):
        arrived(slot, q)
        src = out_ref.at[slot]
        for kind, target in kinds:
            copy(src, slot, kind, q, base + target).start()
        to_halo(slot, src, q)

    for q in range(count + 2):
        if q < count:
            take(first, q, [(3, first_to), (4, mate)])
            take(second, q, [(5, mate)])
            take(mate, q, [])
        if 1 <= q <= count:
            take(diag, q - 1, [(6, mate)])
            take(xor(3), q - 1, [])
            take(xor(5), q - 1, [])
        if q >= 2:
            take(xor(7), q - 2, [])
    for q in range(count):
        arrived(GROUP, q)

        @pl.when(core == 0)
        def _():
            copy(out_ref.at[GROUP], GROUP, 8, q, base + mate).start()

    for c in local:
        c.wait()
    for kind in range(9):
        for q in range(count):
            if kind < 7:
                copy(value_ref, j, kind, q, base + mate).wait_send()
            else:

                @pl.when(core == 0)
                def _():
                    copy(value_ref, j, kind, q, base + mate).wait_send()


def gather(n, low, high, value, *earlier):
    rows, _, nz, nw = value.shape
    count = len(pieces_of(rows, low, high))
    vmem = pl.BlockSpec(memory_space=pltpu.VMEM)
    return pl.pallas_call(
        functools.partial(gather_kernel, n, low, high),
        out_shape=pltpu.VMEM((GROUP + 1, rows, high, nz, nw), value.dtype),
        in_specs=[vmem] * (1 + len(earlier)),
        out_specs=vmem,
        scratch_shapes=[
            pltpu.SemaphoreType.DMA((9, count)),
            pltpu.SemaphoreType.DMA((GROUP + 1, count)),
            pltpu.SemaphoreType.DMA((rows * (GROUP + 2),)),
        ],
        compiler_params=pltpu.CompilerParams(
            collective_id=len(earlier), has_side_effects=True, vmem_limit_bytes=16 * 2**20
        ),
    )(value, *earlier)


def partial_kernel(side, ny, y0, frac, cost, slab_at, cell_at, grid_at, src, before, best, mid, picked):
    rows, planes, nz, nw = best.shape
    j = lax.rem(lax.axis_index("gx"), GROUP)
    controls = cost.shape[0]

    def place(u):
        return j + slab_at[u] + side * GROUP

    def pick(u, m):
        at = place(u)
        inside = jnp.logical_and(at >= 0, at < GROUP)

        @pl.when(inside)
        def _():
            picked[m] = u

        return m + inside.astype(jnp.int32)

    number = lax.fori_loop(0, controls, pick, 0)
    best[...] = jnp.full(best.shape, jnp.inf, jnp.float32)

    def one(i, carry):
        u = picked[i]
        start = place(u) * rows + cell_at[u]
        fx, fy, fz, fw = frac[u, 0], frac[u, 1], frac[u, 2], frac[u, 3]
        gy, gz, gw = grid_at[u, 0], grid_at[u, 1], grid_at[u, 2]
        add = cost[u]
        turn = lax.rem(nw - gw, nw)
        turn1 = lax.rem(nw - gw - 1, nw)

        def row(r, c):
            def along(y):
                y = y + y0 + gy
                y = jnp.where(y >= ny, y - ny, y)
                a = start + r
                low, high = src[a, y], src[a + 1, y]
                return low + fx * (high - low)

            def first(b, low):
                for k in range(UNROLL):
                    y = b * UNROLL + k
                    high = along(y + 1)
                    got = low + fy * (high - low)
                    mid[y, 8:8 + nz] = got
                    mid[y, 0:8] = got[nz - 8:]
                    mid[y, 8 + nz:16 + nz] = got[:8]
                    low = high
                return low

            lax.fori_loop(0, planes // UNROLL, first, along(0))

            def second(b, c2):
                for k in range(UNROLL):
                    y = b * UNROLL + k
                    low = mid[y, pl.ds(8 + gz, nz)]
                    high = mid[y, pl.ds(9 + gz, nz)]
                    got = low + fz * (high - low)
                    low, high = pltpu.roll(got, turn, 1), pltpu.roll(got, turn1, 1)
                    got = low + fw * (high - low) + add
                    best[r, y] = jnp.minimum(best[r, y], got)
                return c2

            lax.fori_loop(0, planes // UNROLL, second, 0)
            return c

        return lax.fori_loop(0, rows, row, carry)

    lax.fori_loop(0, number, one, 0)


def partial(side, ny, y0, planes, src, before, frac, cost, slab_at, cell_at, grid_at):
    _, rows, held, nz, nw = src.shape
    smem = pl.BlockSpec(memory_space=pltpu.SMEM)
    flat = src.reshape((src.shape[0] * rows, held, nz, nw))
    return pl.pallas_call(
        functools.partial(partial_kernel, side, ny, y0),
        out_shape=jax.ShapeDtypeStruct((rows, planes, nz, nw), src.dtype),
        in_specs=[smem] * 5
        + [pl.BlockSpec(memory_space=pltpu.VMEM), pl.BlockSpec(memory_space=pl.ANY)],
        out_specs=pl.BlockSpec(memory_space=pltpu.VMEM),
        scratch_shapes=[
            pltpu.VMEM((planes, nz + 16, nw), jnp.float32),
            pltpu.SMEM((cost.shape[0],), jnp.int32),
        ],
        compiler_params=pltpu.CompilerParams(vmem_limit_bytes=16 * 2**20),
        cost_estimate=pl.CostEstimate(
            flops=12000000, bytes_accessed=8000000, transcendentals=0
        ),
    )(frac, cost, slab_at, cell_at, grid_at, flat, before)


def finish_kernel(target, obstacle, own, *refs):
    pieces, out = refs[:-1], refs[-1]
    rows, ny = own.shape[:2]
    half = ny // 2

    def step(i, c):
        for h in range(2):
            y = i + h * half + SHIFT
            y = jnp.where(y >= ny, y - ny, y)
            for r in range(rows):
                best = own[r, i + h * half]
                for piece in pieces[2 * h : 2 * h + 2]:
                    best = jnp.minimum(best, piece[r, i])
                out[r, y] = jnp.maximum(obstacle[r, y], jnp.minimum(target[r, y], best))
        return c

    lax.fori_loop(0, half, step, 0)


def finish(target, obstacle, own, pieces):
    vmem = pl.BlockSpec(memory_space=pltpu.VMEM)
    return pl.pallas_call(
        finish_kernel,
        out_shape=jax.ShapeDtypeStruct(own.shape, own.dtype),
        in_specs=[vmem] * (3 + len(pieces)),
        out_specs=vmem,
        compiler_params=pltpu.CompilerParams(vmem_limit_bytes=16 * 2**20),
    )(target, obstacle, own, *pieces)


def passed_along(x, by):
    size = lax.axis_size("gx")
    return lax.ppermute(x, "gx", [(i, (i + by) % size) for i in range(size)])


def body(value, target, obstacle, *params):
    n = lax.axis_size("gx")
    ny = value.shape[1]
    half = ny // 2
    early = half + 2 * SHIFT + 1
    src = before = gather(n, 0, early, value)
    sent = []
    for h in range(2):
        if h:
            src = gather(n, early, ny, value, src)
        for side in (-1, 1):
            before = partial(side, ny, SHIFT + h * half, half, src, before, *params)
            sent.append(passed_along(before, side * GROUP))
    own = partial(0, ny, SHIFT, ny, src, before, *params)
    return finish(target, obstacle, own, sent)


def solution(mesh):
    slab = P("gx", None, None, None)
    return jax.shard_map(
        body,
        mesh=mesh,
        in_specs=(slab, slab, slab, P(), P(), P(), P(), P()),
        out_specs=slab,
        check_vma=False,
    )
```

```python
import functools

import jax
import jax.numpy as jnp
from jax import lax
from jax.experimental import pallas as pl
from jax.experimental.pallas import tpu as pltpu
from jax.sharding import PartitionSpec as P


GROUP = 8
MESH = pl.DeviceIdType.MESH
HALVES = 2
UNROLL = 12


def gather_kernel(n, value_ref, out_ref, send_sem, recv_sem, own_sem):
    me = lax.axis_index("gx")
    j = lax.rem(me, GROUP)
    base = me - j
    core = lax.rem(j, 2)

    def xor(bits):
        got = j
        for bit in (1, 2, 4):
            if bits & bit:
                got = got + bit - 2 * bit * lax.rem(got // bit, 2)
        return got

    mate, xn, yn, diag = xor(1), xor(2), xor(4), xor(6)
    first, first_to = jnp.where(core == 0, xn, yn), jnp.where(core == 0, yn, xn)
    second = first_to
    down, up = lax.rem(me + n - GROUP, n), lax.rem(me + GROUP, n)

    barrier = pltpu.get_barrier_semaphore()
    for other in (base + mate, base + xn, base + yn, down, up):
        pl.semaphore_signal(barrier, inc=1, device_id=(other,), device_id_type=MESH)
    pl.semaphore_wait(barrier, 5)

    rows, ny = value_ref.shape[0], value_ref.shape[1]
    part = ny // HALVES
    pieces = [(r, pl.ds(h * part, part)) for r in range(rows) for h in range(HALVES)]
    count = len(pieces)

    def copy(src, slot, kind, q, target):
        r, ys = pieces[q]
        return pltpu.make_async_remote_copy(
            src_ref=src.at[r, ys],
            dst_ref=out_ref.at[slot, r, ys],
            send_sem=send_sem.at[kind, q],
            recv_sem=recv_sem.at[slot, q],
            device_id=(target,),
            device_id_type=MESH,
        )

    def arrived(slot, q):
        r, ys = pieces[q]
        ref = out_ref.at[slot, r, ys]
        pltpu.make_async_copy(ref, ref, recv_sem.at[slot, q]).wait()

    def to_halo(slot, src, q):
        @pl.when(jnp.logical_and(slot == 0, core == 0))
        def _():
            copy(src, GROUP, 7, q, down).start()

    own = pltpu.make_async_copy(value_ref, out_ref.at[j], own_sem)
    for q in range(count):
        copy(value_ref, j, 0, q, base + first).start()
        copy(value_ref, j, 1, q, base + second).start()
        copy(value_ref, j, 2, q, base + mate).start()
        to_halo(j, value_ref, q)
    own.start()

    def take(slot, q, kinds):
        arrived(slot, q)
        src = out_ref.at[slot]
        for kind, target in kinds:
            copy(src, slot, kind, q, base + target).start()
        to_halo(slot, src, q)

    for q in range(count + 2):
        if q < count:
            take(first, q, [(3, first_to), (4, mate)])
            take(second, q, [(5, mate)])
            take(mate, q, [])
        if 1 <= q <= count:
            take(diag, q - 1, [(6, mate)])
            take(xor(3), q - 1, [])
            take(xor(5), q - 1, [])
        if q >= 2:
            take(xor(7), q - 2, [])
    for q in range(count):
        arrived(GROUP, q)

        @pl.when(core == 0)
        def _():
            copy(out_ref.at[GROUP], GROUP, 8, q, base + mate).start()

    own.wait()
    for kind in range(9):
        for q in range(count):
            if kind < 7:
                copy(value_ref, j, kind, q, base + mate).wait_send()
            else:

                @pl.when(core == 0)
                def _():
                    copy(value_ref, j, kind, q, base + mate).wait_send()


def gather(n, value):
    rows = value.shape
    count = rows[0] * HALVES
    return pl.pallas_call(
        functools.partial(gather_kernel, n),
        out_shape=pltpu.VMEM((GROUP + 1,) + rows, value.dtype),
        in_specs=[pl.BlockSpec(memory_space=pltpu.VMEM)],
        out_specs=pl.BlockSpec(memory_space=pltpu.VMEM),
        scratch_shapes=[
            pltpu.SemaphoreType.DMA((9, count)),
            pltpu.SemaphoreType.DMA((GROUP + 1, count)),
            pltpu.SemaphoreType.DMA,
        ],
        compiler_params=pltpu.CompilerParams(
            collective_id=0, has_side_effects=True, vmem_limit_bytes=20 * 2**20
        ),
    )(value)


def partial_kernel(side, rows, row0, frac, cost, slab_at, cell_at, grid_at, src, before, best, mid, picked):
    _, ny, nz, nw = best.shape
    j = lax.rem(lax.axis_index("gx"), GROUP)
    controls = cost.shape[0]

    def place(u):
        return j + slab_at[u] + side * GROUP

    def pick(u, m):
        at = place(u)
        inside = jnp.logical_and(at >= 0, at < GROUP)

        @pl.when(inside)
        def _():
            picked[m] = u

        return m + inside.astype(jnp.int32)

    number = lax.fori_loop(0, controls, pick, 0)
    best[...] = jnp.full(best.shape, jnp.inf, jnp.float32)

    def one(i, carry):
        u = picked[i]
        start = place(u) * rows + cell_at[u] + row0
        fx, fy, fz, fw = frac[u, 0], frac[u, 1], frac[u, 2], frac[u, 3]
        gy, gz, gw = grid_at[u, 0], grid_at[u, 1], grid_at[u, 2]
        add = cost[u]
        turn = lax.rem(nw - gw, nw)
        turn1 = lax.rem(nw - gw - 1, nw)

        def row(r, c):
            def along(y):
                y = y + gy
                y = jnp.where(y < 0, y + ny, y)
                y = jnp.where(y >= ny, y - ny, y)
                low, high = src[start + r, y], src[start + r + 1, y]
                return low + fx * (high - low)

            def first(b, low):
                for k in range(UNROLL):
                    y = b * UNROLL + k
                    high = along(y + 1)
                    got = low + fy * (high - low)
                    mid[y, 8:8 + nz] = got
                    mid[y, 0:8] = got[nz - 8:]
                    mid[y, 8 + nz:16 + nz] = got[:8]
                    low = high
                return low

            lax.fori_loop(0, ny // UNROLL, first, along(0))

            def second(b, c2):
                for k in range(UNROLL):
                    y = b * UNROLL + k
                    low = mid[y, pl.ds(8 + gz, nz)]
                    high = mid[y, pl.ds(9 + gz, nz)]
                    got = low + fz * (high - low)
                    low, high = pltpu.roll(got, turn, 1), pltpu.roll(got, turn1, 1)
                    got = low + fw * (high - low) + add
                    best[r, y] = jnp.minimum(best[r, y], got)
                return c2

            lax.fori_loop(0, ny // UNROLL, second, 0)
            return c

        return lax.fori_loop(0, best.shape[0], row, carry)

    lax.fori_loop(0, number, one, 0)


def partial(side, like, row0, number, src, before, frac, cost, slab_at, cell_at, grid_at):
    rows, ny, nz, nw = like.shape
    smem = pl.BlockSpec(memory_space=pltpu.SMEM)
    flat = src.reshape((src.shape[0] * rows, ny, nz, nw))
    return pl.pallas_call(
        functools.partial(partial_kernel, side, rows, row0),
        out_shape=jax.ShapeDtypeStruct((number, ny, nz, nw), like.dtype),
        in_specs=[smem] * 5
        + [pl.BlockSpec(memory_space=pltpu.VMEM), pl.BlockSpec(memory_space=pl.ANY)],
        out_specs=pl.BlockSpec(memory_space=pltpu.VMEM),
        scratch_shapes=[
            pltpu.VMEM((ny, nz + 16, nw), jnp.float32),
            pltpu.SMEM((cost.shape[0],), jnp.int32),
        ],
        compiler_params=pltpu.CompilerParams(vmem_limit_bytes=20 * 2**20),
        cost_estimate=pl.CostEstimate(
            flops=12000000 * number, bytes_accessed=8000000 * number, transcendentals=0
        ),
    )(frac, cost, slab_at, cell_at, grid_at, flat, before)


def finish_kernel(rows, *refs):
    target, obstacle, own = refs[:3]
    pieces, out = refs[3:-1], refs[-1]

    def step(y, c):
        for r in range(rows):
            best = own[r, y]
            for piece in pieces[r::rows]:
                best = jnp.minimum(best, piece[0, y])
            out[r, y] = jnp.maximum(obstacle[r, y], jnp.minimum(target[r, y], best))
        return c

    lax.fori_loop(0, own.shape[1], step, 0, unroll=4)


def finish(target, obstacle, own, pieces):
    vmem = pl.BlockSpec(memory_space=pltpu.VMEM)
    return pl.pallas_call(
        functools.partial(finish_kernel, own.shape[0]),
        out_shape=jax.ShapeDtypeStruct(own.shape, own.dtype),
        in_specs=[vmem] * (3 + len(pieces)),
        out_specs=vmem,
        compiler_params=pltpu.CompilerParams(vmem_limit_bytes=20 * 2**20),
    )(target, obstacle, own, *pieces)


def passed_along(x, by):
    size = lax.axis_size("gx")
    return lax.ppermute(x, "gx", [(i, (i + by) % size) for i in range(size)])


def body(value, target, obstacle, *params):
    n = lax.axis_size("gx")
    src = gather(n, value)
    rows = value.shape[0]
    before = value
    sent = {-1: [], 1: []}
    for r in range(rows):
        for side in sent:
            before = partial(side, value, r, 1, src, before, *params)
            sent[side].append(passed_along(before, side * GROUP))
    own = partial(0, value, 0, rows, src, before, *params)
    return finish(target, obstacle, own, sent[-1] + sent[1])


def solution(mesh):
    slab = P("gx", None, None, None)
    return jax.shard_map(
        body,
        mesh=mesh,
        in_specs=(slab, slab, slab, P(), P(), P(), P(), P()),
        out_specs=slab,
        check_vma=False,
    )
```
